32 devices in a mesh: expert: 4 (over x, core), shard: 8 (over z, y).
Axes of the slice: x: 2, y: 2, z: 4, core: 2. Of those that a mesh axis runs over, the one named last changes fastest.
Arguments:
- w_gate: float32 [64, 2048, 1408], P('expert', 'shard'), may hold values from -0.1875 to 0.1875
- w_up: float32 [64, 2048, 1408], P('expert', 'shard'), may hold values from -0.1875 to 0.1875
- router_weight: float32 [2048, 64], P('shard', 'expert'), may hold values from -0.125 to 0.125
- router_gain: float32 [2048], P('shard'), may hold values from 0.25 to 1.75
Outputs:
- serve_gate: bfloat16 [64, 2048, 1408], P('expert', None, 'shard')
- serve_up: bfloat16 [64, 2048, 1408], P('expert', None, 'shard')
- scale_gate: float32 [64, 1408], P('expert', 'shard')
- scale_up: float32 [64, 1408], P('expert', 'shard')
- serve_router: bfloat16 [2048, 64], replicated
The draws below stay inside these ranges and needn't reach their ends.
All inputs are finite; a program needn't handle non-finite values. Where the reference program divides by a largest or mean magnitude, that divisor is 1e-20 or more.
Results may differ from the reference program's by a relative error of at most 0.001.
Values may be sent and summed in bfloat16 or wider, within the bound.
A program may use at most 192 MiB of HBM per device.

```python
import jax
import jax.numpy as jnp

EXPERTS = 64
D_MODEL = 2048
D_EXPERT = 1408


def raised(result, key, source, target, parts, factor):
    owner, partner = [(jnp.arange(result.shape[dim]) // (result.shape[dim] // parts)).reshape([-1 if axis == dim else 1 for axis in range(result.ndim)]) for dim in (source, target)]
    chosen = jax.random.permutation(key, parts)[partner]
    strong = (owner == chosen) | (owner == (partner + parts // 2) % parts)
    return jnp.where(strong, factor * result, result)


def block_levels(rng, shape, split, least, high):
    factor_of, own = 1.0, jax.random.fold_in(rng, 6)
    for position, parts in split:
        draws = jnp.exp(jax.random.uniform(jax.random.fold_in(own, position), (parts,), jnp.float32, least / len(split), high / len(split)))
        factor_of = factor_of * jnp.repeat(draws, shape[position] // parts).reshape([-1 if axis == position else 1 for axis in range(len(shape))])
    return factor_of


def normal_values(stream_key, extent, spread, most, cuts=(), dtype=jnp.bfloat16):
    values = jax.random.normal(stream_key, extent, jnp.float32) * spread
    if len(cuts) > 0:
        values = block_levels(stream_key, extent, cuts, -0.22, 0.18) * values
    return jnp.clip(values, min=-most, max=most).astype(dtype)


def gaussian_with(stream_key, shape, deviation, limit, shards, heavy, held_as=jnp.bfloat16):
    entries = deviation * jax.random.normal(stream_key, shape, jnp.float32)
    if shards:
        entries = entries * block_levels(stream_key, shape, shards, -0.22, 0.18)
    return jnp.clip(raised(entries, jax.random.fold_in(stream_key, 3), *heavy), -limit, limit).astype(held_as)


def setup_inputs(seed: int = 0) -> dict:
    key_list = jax.random.split(jax.random.key(seed), 5)
    return {
        "w_gate": gaussian_with(key_list[0], (EXPERTS, D_MODEL, D_EXPERT), D_MODEL ** -0.5, 0.1875, ((0, 4), (1, 8)), (1, 2, 8, 2.0), jnp.float32),
        "w_up": gaussian_with(key_list[1], (EXPERTS, D_MODEL, D_EXPERT), D_MODEL ** -0.5, 0.1875, ((0, 4), (1, 8)), (1, 2, 8, 2.0), jnp.float32),
        "router_weight": normal_values(key_list[2], (D_MODEL, EXPERTS), D_MODEL ** -0.5, 0.125, ((0, 8), (1, 4)), jnp.float32),
        "router_gain": jnp.clip(1.0 + 0.15 * jax.random.normal(key_list[3], (D_MODEL,), jnp.float32), 0.25, 1.75),
    }


def reference(w_gate, w_up, router_weight, router_gain):
    scale_gate = jnp.sum(jnp.abs(w_gate), axis=1) / D_MODEL
    serve_gate = (w_gate / jnp.expand_dims(scale_gate, 1)).astype(jnp.bfloat16)
    scale_up = jnp.sum(jnp.abs(w_up), axis=1) / D_MODEL
    serve_up = (w_up / jnp.expand_dims(scale_up, 1)).astype(jnp.bfloat16)
    serve_router = (router_weight * router_gain[:, None]).astype(jnp.bfloat16)
    return serve_gate, serve_up, scale_gate, scale_up, serve_router
```

```python
import functools

import jax
import jax.numpy as jnp
from jax import lax
from jax.experimental import pallas as pl
from jax.experimental.pallas import tpu as pltpu
from jax.sharding import PartitionSpec as P

LANES = 128
SLOTS = 2


def plain(w_gate, w_up, router_weight, router_gain):
    model = w_gate.shape[1] * lax.axis_size("shard")
    total_gate, total_up = lax.psum(
        (jnp.sum(jnp.abs(w_gate), axis=1), jnp.sum(jnp.abs(w_up), axis=1)), "shard"
    )
    served = []
    scales = []
    for w, total in ((w_gate, total_gate), (w_up, total_up)):
        scale = total / model
        narrow = (w / jnp.expand_dims(scale, 1)).astype(jnp.bfloat16)
        out = lax.all_to_all(narrow, "shard", split_axis=2, concat_axis=1, tiled=True)
        served.append(out)
        scales.append(
            lax.dynamic_slice_in_dim(
                scale, lax.axis_index("shard") * out.shape[2], out.shape[2], axis=1
            )
        )
    part_router = (router_weight * router_gain[:, None]).astype(jnp.bfloat16)
    row_router = lax.all_gather(part_router, "shard", axis=0, tiled=True)
    serve_router = lax.all_gather(row_router, "expert", axis=1, tiled=True)
    return (*served, *scales, serve_router)


def kernel(
    n, groups, model,
    part_ref, router_ref, gate_ref, up_ref,
    out_gate, out_up, scale_ref, out_router,
    stage, loaded, arrived, block,
    load_sem, own_sem, sum_send, sum_recv, mean_send, mean_recv,
    col_send, col_recv, row_send, row_recv, data_send, data_recv,
):
    me = lax.axis_index("shard")
    group = lax.axis_index("expert")
    tasks, tiles, _ = part_ref.shape
    experts, rows, width = gate_ref.shape
    columns = width // n
    share = tasks // n
    heads = router_ref.shape[0]

    def to(p):
        return lax.rem(me + p, n)

    def source(p):
        return lax.rem(me + n - p, n)

    def load(w_ref, e, slot):
        return pltpu.make_async_copy(w_ref.at[e], loaded.at[slot], load_sem.at[slot])

    load(gate_ref, 0, 0).start()

    barrier = pltpu.get_barrier_semaphore()
    for p in range(1, n):
        pl.semaphore_signal(barrier, inc=1, device_id={"shard": to(p)})
    for q in range(1, groups):
        pl.semaphore_signal(
            barrier, inc=1, device_id={"expert": lax.rem(group + q, groups)}
        )
    pl.semaphore_wait(barrier, n - 1 + groups - 1)

    sums = []
    for p in range(1, n):
        copy = pltpu.make_async_remote_copy(
            src_ref=part_ref.at[pl.ds(to(p) * share, share)],
            dst_ref=arrived.at[p],
            send_sem=sum_send.at[p],
            recv_sem=sum_recv.at[p],
            device_id={"shard": to(p)},
        )
        copy.start()
        sums.append(copy)

    mine = pl.ds(pl.multiple_of(group * heads, heads), heads)
    block[mine, :] = router_ref[...]
    cols = []
    for q in range(1, groups):
        copy = pltpu.make_async_remote_copy(
            src_ref=router_ref,
            dst_ref=block.at[mine],
            send_sem=col_send.at[q],
            recv_sem=col_recv.at[q],
            device_id={"expert": lax.rem(group + q, groups)},
        )
        copy.start()
        cols.append(copy)

    total = part_ref[pl.ds(me * share, share)]
    for p in range(1, n):
        sums[p - 1].wait_recv()
        total = total + arrived[p]
    own = pl.ds(me * share, share)
    scale_ref[own] = total / model
    means = []
    for p in range(1, n):
        copy = pltpu.make_async_remote_copy(
            src_ref=scale_ref.at[own],
            dst_ref=scale_ref.at[own],
            send_sem=mean_send.at[p],
            recv_sem=mean_recv.at[p],
            device_id={"shard": to(p)},
        )
        copy.start()
        means.append(copy)
    for copy in means:
        copy.wait_recv()

    my_rows = pl.ds(pl.multiple_of(me * rows, rows), rows)

    def piece(k):
        return pl.ds(pl.multiple_of(k * columns, 16), columns)

    order = list(range(1, n))
    for w, (w_ref, out) in enumerate(((gate_ref, out_gate), (up_ref, out_up))):

        def step(e, carry, w=w, w_ref=w_ref, out=out):
            slot = lax.rem(e, SLOTS)
            task = w * experts + e

            @pl.when(e + 1 < experts)
            def _():
                load(w_ref, e + 1, lax.rem(e + 1, SLOTS)).start()

            load(w_ref, e, slot).wait()
            for t in range(tiles):
                lanes = slice(t * LANES, (t + 1) * LANES)
                inverse = 1.0 / scale_ref[task, t : t + 1, :]
                scaled = loaded[slot, :, lanes] * inverse
                stage[task, lanes, :] = scaled.T.astype(jnp.bfloat16)
            for p in order:
                pltpu.make_async_remote_copy(
                    src_ref=stage.at[task, piece(to(p))],
                    dst_ref=out.at[e, :, my_rows],
                    send_sem=data_send.at[w, p],
                    recv_sem=data_recv.at[w, p],
                    device_id={"shard": to(p)},
                ).start()
            pltpu.make_async_copy(
                stage.at[task, piece(me)], out.at[e, :, my_rows], own_sem.at[w]
            ).start()
            return carry

        lax.fori_loop(0, experts, step, 0)
        if w == 0:
            load(up_ref, 0, 0).start()
            for copy in cols:
                copy.wait_recv()
            lines = []
            for p in range(1, n):
                copy = pltpu.make_async_remote_copy(
                    src_ref=block,
                    dst_ref=out_router.at[:, my_rows],
                    send_sem=row_send.at[p],
                    recv_sem=row_recv.at[p],
                    device_id={"shard": to(p)},
                )
                copy.start()
                lines.append(copy)
            out_router[:, my_rows] = block[...]

    for copy in sums + cols + means:
        copy.wait_send()
    for copy in lines:
        copy.wait()
    for w, out in enumerate((out_gate, out_up)):
        held = pl.ds(w * experts, experts)
        pltpu.make_async_copy(
            stage.at[held, piece(me)], out.at[:, :, my_rows], own_sem.at[w]
        ).wait()
        for p in range(1, n):
            from_p = pl.ds(pl.multiple_of(source(p) * rows, rows), rows)
            both = pltpu.make_async_remote_copy(
                src_ref=stage.at[held, piece(to(p))],
                dst_ref=out.at[:, :, from_p],
                send_sem=data_send.at[w, p],
                recv_sem=data_recv.at[w, p],
                device_id={"shard": to(p)},
            )
            both.wait_send()
            both.wait_recv()


def on_device(w_gate, w_up, router_weight, router_gain):
    n, groups = lax.axis_size("shard"), lax.axis_size("expert")
    experts, rows, width = w_gate.shape
    heads = router_weight.shape[1]
    tasks, columns, model = 2 * experts, width // n, rows * n
    if rows % LANES or width % LANES or columns % 16 or tasks % n or heads % 16:
        return plain(w_gate, w_up, router_weight, router_gain)
    tiles = width // LANES
    part = jnp.concatenate(
        [jnp.sum(jnp.abs(w_gate), axis=1), jnp.sum(jnp.abs(w_up), axis=1)]
    ).reshape(tasks, tiles, LANES)
    part_router = (router_weight * router_gain[:, None]).astype(jnp.bfloat16).T
    vmem = pl.BlockSpec(memory_space=pltpu.VMEM)
    hbm = pl.BlockSpec(memory_space=pl.ANY)
    dma = pltpu.SemaphoreType.DMA
    out_gate, out_up, scale, router = pl.pallas_call(
        functools.partial(kernel, n, groups, model),
        out_shape=(
            jax.ShapeDtypeStruct((experts, columns, model), jnp.bfloat16),
            jax.ShapeDtypeStruct((experts, columns, model), jnp.bfloat16),
            jax.ShapeDtypeStruct((tasks, tiles, LANES), jnp.float32),
            jax.ShapeDtypeStruct((heads * groups, model), jnp.bfloat16),
        ),
        in_specs=[vmem, vmem, hbm, hbm],
        out_specs=(hbm, hbm, vmem, vmem),
        scratch_shapes=[
            pltpu.VMEM((tasks, width, rows), jnp.bfloat16),
            pltpu.VMEM((SLOTS, rows, width), jnp.float32),
            pltpu.VMEM((n, tasks // n, tiles, LANES), jnp.float32),
            pltpu.VMEM((heads * groups, rows), jnp.bfloat16),
            dma((SLOTS,)),
            dma((2,)),
            dma((n,)), dma((n,)),
            dma((n,)), dma((n,)),
            dma((groups,)), dma((groups,)),
            dma((n,)), dma((n,)),
            dma((2, n)), dma((2, n)),
        ],
        compiler_params=pltpu.CompilerParams(
            collective_id=0, has_side_effects=True, vmem_limit_bytes=56 * 2**20
        ),
    )(part, part_router, w_gate, w_up)
    mine = lax.dynamic_slice_in_dim(
        scale.reshape(tasks, width), lax.axis_index("shard") * columns, columns, axis=1
    )
    return (
        out_gate.swapaxes(1, 2),
        out_up.swapaxes(1, 2),
        mine[:experts],
        mine[experts:],
        router.T,
    )


def solution(mesh):
    placed = (
        P("expert", "shard", None),
        P("expert", "shard", None),
        P("shard", "expert"),
        P("shard"),
    )
    return jax.shard_map(
        on_device,
        mesh=mesh,
        in_specs=placed,
        out_specs=(
            P("expert", None, "shard"),
            P("expert", None, "shard"),
            P("expert", "shard"),
            P("expert", "shard"),
            P(),
        ),
        check_vma=False,
    )
```
